128 devices in a mesh: grp: 4 (over y_lo, core), dev: 32 (over z, x, y_hi).
Axes of the slice: x: 4, y: 4 (y_hi: 2, y_lo: 2; y = y_hi * 2 + y_lo), z: 4, core: 2. Of those that a mesh axis runs over, the one named last changes fastest.
Arguments:
- targets: float32 [64, 65536], P(None, ('grp', 'dev')), may hold values from -1.7 to 1.7
- source_grid: int32 [64, 16384], P(None, ('grp', 'dev')), may hold values from -1331000 to 1331000
- source_weight: int32 [1, 16384], P(None, ('grp', 'dev')), may hold values from 1 to 1024
Outputs:
- kernel_sum: float32 [65536], P(('grp', 'dev'))
The draws below stay inside these ranges and needn't reach their ends.
All inputs are finite; a program needn't handle non-finite values.
Results may differ from the reference program's by a relative error of at most 0.00017.
Values sent between devices are 32-bit elements; how exact they have to be, the bound alone decides.
No kernel may reach another device: no remote copies, remote signals or barrier semaphores. Data moves between devices by JAX's collectives and lax.ppermute only.
A program may use at most 64 MiB of HBM per device.

```python
import jax
import jax.numpy as jnp
from jax import lax

D = 64
TGT_DEV = 512
SRC_DEV = 128
TARGETS = 65536
SOURCES = 16384
N_DEV = 32


def centre_table(key):
    centre_count = max(SOURCES // SRC_DEV, 1)
    return jax.random.randint(jax.random.fold_in(key, 11), (D, centre_count), -495000, 495001)


def draw_source_grid(key, part):
    centre_count = max(SOURCES // SRC_DEV, 1)
    centres = centre_table(key)
    owner = jax.random.permutation(jax.random.fold_in(key, 12), SOURCES) % centre_count
    first_noise = jax.random.randint(jax.random.fold_in(key, 13), (D, SOURCES), -418000, 418001)
    second_noise = jax.random.randint(jax.random.fold_in(key, 14), (D, SOURCES), -418000, 418001)
    return (centres[:, owner] + first_noise + second_noise).astype(jnp.int32)


def draw_targets(key, part):
    centre_count = max(SOURCES // SRC_DEV, 1)
    centres = centre_table(key).astype(jnp.float32) / 1048576.0
    owner = jax.random.randint(jax.random.fold_in(key, 15), (TARGETS,), 0, centre_count)
    base = centres[:, owner]
    noise = jnp.clip(0.326 * jax.random.normal(jax.random.fold_in(key, 17), (D, TARGETS), jnp.float32), -1.2, 1.2)
    return (base + noise).astype(jnp.float32)


def place_ends(values, key, smallest, top_value):
    index_at = [jax.random.randint(jax.random.fold_in(key, axis), (), 0, length) for axis, length in enumerate(values.shape)]
    widest = values.shape.index(max(values.shape))
    neighbour = index_at[:widest] + [(index_at[widest] + 1) % values.shape[widest]] + index_at[widest + 1:]
    return values.at[tuple(index_at)].set(smallest).at[tuple(neighbour)].set(top_value)


def setup_inputs(seed: int = 0) -> dict:
    arg_keys = jax.random.split(jax.random.key(seed), 4)
    return {
        "targets": draw_targets(jax.random.fold_in(arg_keys[3], 71), 0),
        "source_grid": draw_source_grid(jax.random.fold_in(arg_keys[3], 71), 0),
        "source_weight": place_ends(jax.random.randint(arg_keys[2], (1, SOURCES), 1, 1025), jax.random.fold_in(arg_keys[2], 1), 1, 1024).astype(jnp.int32),
    }


KERNEL_RATE = 0.7


def block_sum(tgt_rows, src_points, src_mass):
    tgt_norm = jnp.sum(tgt_rows * tgt_rows, axis=0)
    src_norm = jnp.sum(src_points * src_points, axis=0)
    inner_prod = lax.dot_general(tgt_rows, src_points, (((0,), (0,)), ((), ())), precision=lax.Precision.HIGHEST, preferred_element_type=jnp.float32)
    distance = tgt_norm[:, None] + src_norm[None, :] - 2.0 * inner_prod
    kernel = jnp.exp(-KERNEL_RATE * distance)
    return jnp.dot(kernel, src_mass[0], precision=lax.Precision.HIGHEST, preferred_element_type=jnp.float32)


def reference(targets, source_grid, source_weight):
    points = source_grid.astype(jnp.float32) / 1048576.0
    masses = source_weight.astype(jnp.float32) / 16.0
    rows_block = TGT_DEV * min(8, N_DEV)
    cols_block = SRC_DEV * 4
    count_cols = SOURCES // cols_block
    point_blocks = jnp.transpose(points.reshape(D, count_cols, cols_block), (1, 0, 2))
    mass_blocks = jnp.transpose(masses.reshape(1, count_cols, cols_block), (1, 0, 2))
    target_blocks = jnp.transpose(targets.reshape(D, TARGETS // rows_block, rows_block), (1, 0, 2))

    def one_target_block(tgt_rows):
        def advance(running, source_pair):
            return running + block_sum(tgt_rows, source_pair[0], source_pair[1]), None
        result, unused = lax.scan(advance, jnp.zeros((rows_block,), jnp.float32), (point_blocks, mass_blocks))
        return result

    sums = lax.map(one_target_block, target_blocks)
    return sums.reshape(TARGETS)
```

```python
import functools
import math

import jax
import jax.numpy as jnp
from jax import lax
from jax.experimental import pallas as pl
from jax.experimental.pallas import tpu as pltpu
from jax.sharding import Mesh, PartitionSpec as P

KERNEL_RATE = 0.7
RATE2 = KERNEL_RATE * math.log2(math.e)
NAMES = ("ylo", "core", "z", "x", "yhi")
BF16 = jnp.bfloat16
F32 = jnp.float32
CHUNK = 256


def y_place(y):
    return (y % 2) * 2 + y // 2


def along_y(block, distance):
    route = [(y_place(y), y_place((y + distance) % 4)) for y in range(4)]
    return lax.ppermute(block, ("ylo", "yhi"), route)


def digits(a):
    high = a.astype(BF16)
    rest = a - high.astype(F32)
    mid = rest.astype(BF16)
    low = (rest - mid.astype(F32)).astype(BF16)
    return high, mid, low


def widened(parts):
    return jnp.concatenate([p.astype(F32) for p in parts], axis=0).astype(BF16)


def sums_kernel(s_ref, t0_ref, t1_ref, t2_ref, t3_ref, o_ref, left, right):
    blocks = s_ref.shape[0]

    def prepare(b, unused):
        points = s_ref[b, :64]
        offset = s_ref[b, 64:65]
        high, mid, low = digits(points)
        extra = widened(digits(offset) + (jnp.ones((3, 128), F32), jnp.zeros((58, 128), F32)))
        stack = jnp.concatenate(
            [high, high, mid, mid, high, low, extra, jnp.zeros((64, 128), BF16)], axis=0
        )
        left[pl.ds(pl.multiple_of(b * 128, 128), 128), :] = stack.T
        return 0

    lax.fori_loop(0, blocks, prepare, 0)
    for k, t_ref in enumerate((t0_ref, t1_ref, t2_ref, t3_ref)):
        tgt = t_ref[...]
        offset = -RATE2 * jnp.sum(tgt * tgt, axis=0, keepdims=True)
        high, mid, low = digits(tgt * (2 * RATE2))
        extra = widened((jnp.ones((3, 512), F32),) + digits(offset) + (jnp.zeros((58, 512), F32),))
        right[:, k * 512 : (k + 1) * 512] = jnp.concatenate(
            [high, mid, high, mid, low, high, extra, jnp.zeros((64, 512), BF16)], axis=0
        )

    def tile(n, unused):
        at = pl.multiple_of(n * 256, 256)
        weights = right[:, pl.ds(at, 256)]
        total = jnp.zeros((8, 256), F32)
        for m in range(blocks * 128 // CHUNK):
            power = jnp.dot(
                left[m * CHUNK : (m + 1) * CHUNK, :], weights, preferred_element_type=F32
            )
            total = total + jnp.sum(jnp.exp2(power).reshape(CHUNK // 8, 8, 256), axis=0)
        o_ref[:, pl.ds(at, 256)] = jnp.sum(total, axis=0, keepdims=True)
        return 0

    lax.fori_loop(0, 8, tile, 0)


def partial_sums(sources, tgts):
    blocks = sources.shape[0]
    return pl.pallas_call(
        sums_kernel,
        out_shape=jax.ShapeDtypeStruct((1, 2048), F32),
        in_specs=[pl.BlockSpec(memory_space=pltpu.VMEM)] * 5,
        out_specs=pl.BlockSpec(memory_space=pltpu.VMEM),
        scratch_shapes=[pltpu.VMEM((blocks * 128, 512), BF16), pltpu.VMEM((512, 2048), BF16)],
        cost_estimate=pl.CostEstimate(
            flops=2 * blocks * 128 * 2048 * 512, bytes_accessed=1 << 20, transcendentals=0
        ),
        name="partial_sums",
    )(sources, *tgts)


def shards(targets, source_grid, source_weight):
    tgts = [targets] + [along_y(targets, k) for k in (1, 3, 2)]
    points = source_grid.astype(F32) / 1048576.0
    masses = source_weight.astype(F32) / 16.0
    offset = jnp.log2(masses) - RATE2 * jnp.sum(points * points, axis=0, keepdims=True)
    payload = jnp.concatenate([points, offset, jnp.zeros((7, points.shape[1]), F32)], axis=0)
    spread = jnp.broadcast_to(payload[None], (16,) + payload.shape)
    near = lax.all_to_all(spread, ("z", "x"), 0, 0, tiled=True)
    far = lax.ppermute(near, "core", [(0, 1), (1, 0)])
    sums = partial_sums(near, tgts) + partial_sums(far, tgts)
    parts = sums.reshape(4, 512)
    total = parts[0]
    for part, k in zip((parts[1], parts[2], parts[3]), (3, 1, 2)):
        total = total + along_y(part, k)
    return total


def solution(mesh):
    torus = Mesh(mesh.devices.reshape(2, 2, 4, 4, 2), NAMES)
    specs = (P(None, NAMES),) * 3
    return jax.shard_map(shards, mesh=torus, in_specs=specs, out_specs=P(NAMES), check_vma=False)
```

```python
import math

import jax
import jax.numpy as jnp
from jax import lax
from jax.experimental import pallas as pl
from jax.experimental.pallas import tpu as pltpu
from jax.sharding import Mesh, PartitionSpec as P


KERNEL_RATE = 0.7
RATE2 = KERNEL_RATE * math.log2(math.e)
NAMES = ("ylo", "core", "z", "x", "yhi")
BF16 = jnp.bfloat16
F32 = jnp.float32
CHUNK = 256
BLOCKS = 16
ROWS = BLOCKS * 128
SHIFTS = (1, 3, 2)


def y_place(y):
    return (y % 2) * 2 + y // 2


def along_y(block, distance):
    route = [(y_place(y), y_place((y + distance) % 4)) for y in range(4)]
    return lax.ppermute(block, ("ylo", "yhi"), route)


def digits(a):
    high = a.astype(BF16)
    rest = a - high.astype(F32)
    mid = rest.astype(BF16)
    low = (rest - mid.astype(F32)).astype(BF16)
    return high, mid, low


def widened(parts):
    return jnp.concatenate([p.astype(F32) for p in parts], axis=0).astype(BF16)


def prepare_left(s_ref, left):
    def prepare(b, unused):
        high, mid, low = digits(s_ref[b, :64])
        offset = digits(s_ref[b, 64:65])
        extra = widened(offset + (jnp.ones((3, 128), F32), jnp.zeros((58, 128), F32)))
        rows = pl.ds(pl.multiple_of(b * 128, 128), 128)
        left[rows, :128] = jnp.concatenate([high, mid], axis=0).T
        left[rows, 128:] = jnp.concatenate([low, extra], axis=0).T
        return 0

    lax.fori_loop(0, BLOCKS, prepare, 0, unroll=2)


def prepare_right(t_ref, right, at):
    tgt = t_ref[...]
    width = tgt.shape[1]
    offset = -RATE2 * jnp.sum(tgt * tgt, axis=0, keepdims=True)
    high, mid, low = digits(tgt * (2 * RATE2))
    extra = widened((jnp.ones((3, width), F32),) + digits(offset) + (jnp.zeros((58, width), F32),))
    empty = jnp.zeros((64, width), BF16)
    right[:, at : at + width] = jnp.concatenate(
        [high, high, mid, mid, low, empty, high, extra], axis=0
    )


def column_sums(lefts, weights):
    total = jnp.zeros((8, weights.shape[1]), F32)
    for left in lefts:
        for m in range(ROWS // CHUNK):
            rows = slice(m * CHUNK, (m + 1) * CHUNK)
            first, second = left[rows, :128], left[rows, 128:]
            power = jnp.dot(
                jnp.concatenate([first, first, first, second], axis=1),
                weights,
                preferred_element_type=F32,
            )
            total = total + jnp.sum(jnp.exp2(power).reshape(CHUNK // 8, 8, -1), axis=0)
    return jnp.sum(total, axis=0, keepdims=True)


def near_kernel(s_ref, t1_ref, t2_ref, t3_ref, part, left, right):
    prepare_left(s_ref, left)
    for k, t_ref in enumerate((t1_ref, t2_ref, t3_ref)):
        prepare_right(t_ref, right, k * 512)

    def tile(n, unused):
        cols = pl.ds(pl.multiple_of(n * 256, 256), 256)
        part[:, cols] = column_sums((left,), right[:, cols])
        return 0

    lax.fori_loop(0, 6, tile, 0)


def far_kernel(s_ref, right, part, o1, o2, o3, left):
    prepare_left(s_ref, left)
    for k, o_ref in enumerate((o1, o2, o3)):

        def tile(n, unused):
            out = pl.ds(pl.multiple_of(n * 256, 256), 256)
            cols = pl.ds(pl.multiple_of(n * 256 + k * 512, 256), 256)
            o_ref[:, out] = part[:, cols] + column_sums((left,), right[:, cols])
            return 0

        lax.fori_loop(0, 2, tile, 0)


def own_kernel(near, far, t_ref, out, right):
    prepare_right(t_ref, right, 0)

    def tile(n, unused):
        cols = pl.ds(pl.multiple_of(n * 256, 256), 256)
        out[:, cols] = column_sums((near, far), right[:, cols])
        return 0

    lax.fori_loop(0, 2, tile, 0)


def run(body, tiles, outs, args, scratch=()):
    vmem = pl.BlockSpec(memory_space=pltpu.VMEM)
    return pl.pallas_call(
        body,
        out_shape=[jax.ShapeDtypeStruct(*o) for o in outs],
        in_specs=[vmem] * len(args),
        out_specs=[vmem] * len(outs),
        scratch_shapes=list(scratch),
        compiler_params=pltpu.CompilerParams(vmem_limit_bytes=16 << 20),
        cost_estimate=pl.CostEstimate(
            flops=2 * ROWS * 256 * 512 * tiles, bytes_accessed=1 << 20, transcendentals=0
        ),
    )(*args)


def shards(targets, source_grid, source_weight):
    tgts = []
    for k in SHIFTS:
        tgts.append(along_y(targets, k))
    points = source_grid.astype(F32) / 1048576.0
    masses = source_weight.astype(F32) / 16.0
    offset = jnp.log2(masses) - RATE2 * jnp.sum(points * points, axis=0, keepdims=True)
    payload = jnp.concatenate([points, offset, jnp.zeros((7, points.shape[1]), F32)], axis=0)
    spread = jnp.broadcast_to(payload[None], (BLOCKS,) + payload.shape)
    near = lax.all_to_all(spread, ("z", "x"), 0, 0, tiled=True)
    far = lax.ppermute(near, "core", [(0, 1), (1, 0)])
    stack = ((ROWS, 256), BF16)
    part, near_left, right = run(
        near_kernel, 6, [((1, 1536), F32), stack, ((512, 1536), BF16)],
        (near, *tgts),
    )
    *parts, far_left = run(far_kernel, 6, [((1, 512), F32)] * 3 + [stack], (far, right, part))
    total = run(
        own_kernel, 4, [((1, 512), F32)], (near_left, far_left, targets),
        [pltpu.VMEM((512, 512), BF16)],
    )[0]
    for part, k in zip(parts, SHIFTS):
        part = along_y(part, 4 - k)
        total = total + part
    return total.reshape(512)


def solution(mesh):
    torus = Mesh(mesh.devices.reshape(2, 2, 4, 4, 2), NAMES)
    specs = (P(None, NAMES),) * 3
    return jax.shard_map(shards, mesh=torus, in_specs=specs, out_specs=P(NAMES), check_vma=False)
```

```python
import math

import jax
import jax.numpy as jnp
from jax import lax
from jax.experimental import pallas as pl
from jax.experimental.pallas import tpu as pltpu
from jax.sharding import Mesh, PartitionSpec as P


KERNEL_RATE = 0.7
RATE2 = KERNEL_RATE * math.log2(math.e)
NAMES = ("ylo", "core", "z", "x", "yhi")
BF16 = jnp.bfloat16
F32 = jnp.float32
CHUNK = 256
TILE = 256
BLOCKS = 16
ROWS = BLOCKS * 128
SHIFTS = (1, 3, 2)


def y_place(y):
    return (y % 2) * 2 + y // 2


def along_y(block, distance):
    route = [(y_place(y), y_place((y + distance) % 4)) for y in range(4)]
    return lax.ppermute(block, ("ylo", "yhi"), route)


def digits(a):
    high = a.astype(BF16)
    rest = a - high.astype(F32)
    mid = rest.astype(BF16)
    low = (rest - mid.astype(F32)).astype(BF16)
    return high, mid, low


def widened(parts):
    return jnp.concatenate([p.astype(F32) for p in parts], axis=0).astype(BF16)


def prepare_left(s_ref, b, left):
    high, mid, low = digits(s_ref[b, :64])
    offset = digits(s_ref[b, 64:65])
    extra = widened(offset + (jnp.ones((3, 128), F32), jnp.zeros((58, 128), F32)))
    rows = slice(b * 128, (b + 1) * 128)
    left[rows, :128] = jnp.concatenate([high, mid], axis=0).T
    left[rows, 128:] = jnp.concatenate([low, extra], axis=0).T


def prepare_right(t_ref, n, right, cols):
    tgt = t_ref[:, n * TILE : (n + 1) * TILE]
    offset = -RATE2 * jnp.sum(tgt * tgt, axis=0, keepdims=True)
    high, mid, low = digits(tgt * (2 * RATE2))
    extra = widened((jnp.ones((3, TILE), F32),) + digits(offset) + (jnp.zeros((58, TILE), F32),))
    empty = jnp.zeros((64, TILE), BF16)
    right[:, cols] = jnp.concatenate([high, high, mid, mid, low, empty, high, extra], axis=0)


def column_sums(lefts, weights, prepare=None):
    total = jnp.zeros((8, TILE), F32)
    for left in lefts:
        for m in range(ROWS // CHUNK):
            if prepare is not None:
                for b in range(m * CHUNK // 128, (m + 1) * CHUNK // 128):
                    prepare(b)
            rows = slice(m * CHUNK, (m + 1) * CHUNK)
            first, second = left[rows, :128], left[rows, 128:]
            power = jnp.dot(
                jnp.concatenate([first, first, first, second], axis=1),
                weights,
                preferred_element_type=F32,
            )
            total = total + jnp.sum(jnp.exp2(power).reshape(CHUNK // 8, 8, TILE), axis=0)
    return jnp.sum(total, axis=0, keepdims=True)


def near_kernel(s_ref, t1_ref, t2_ref, t3_ref, part, left, right):
    for tile in range(6):
        cols = slice(tile * TILE, (tile + 1) * TILE)
        prepare_right((t1_ref, t2_ref, t3_ref)[tile // 2], tile % 2, right, cols)
        prepare = (lambda b: prepare_left(s_ref, b, left)) if tile == 0 else None
        part[:, cols] = column_sums((left,), right[:, cols], prepare)


def far_kernel(s_ref, right, part, o1, o2, o3, left):
    for tile in range(6):
        cols = slice(tile * TILE, (tile + 1) * TILE)
        out = slice(tile % 2 * TILE, (tile % 2 + 1) * TILE)
        prepare = (lambda b: prepare_left(s_ref, b, left)) if tile == 0 else None
        sums = column_sums((left,), right[:, cols], prepare)
        (o1, o2, o3)[tile // 2][:, out] = part[:, cols] + sums


def own_kernel(near, far, t_ref, out, right):
    for tile in range(2):
        cols = slice(tile * TILE, (tile + 1) * TILE)
        prepare_right(t_ref, tile, right, cols)
        out[:, cols] = column_sums((near, far), right[:, cols])


def run(body, tiles, outs, args, scratch=()):
    vmem = pl.BlockSpec(memory_space=pltpu.VMEM)
    return pl.pallas_call(
        body,
        out_shape=[jax.ShapeDtypeStruct(*o) for o in outs],
        in_specs=[vmem] * len(args),
        out_specs=[vmem] * len(outs),
        scratch_shapes=list(scratch),
        compiler_params=pltpu.CompilerParams(vmem_limit_bytes=16 << 20),
        cost_estimate=pl.CostEstimate(
            flops=2 * ROWS * 256 * 512 * tiles, bytes_accessed=1 << 20, transcendentals=0
        ),
    )(*args)


def shards(targets, source_grid, source_weight):
    tgts = []
    for k in SHIFTS:
        tgts.append(along_y(targets, k))
    points = source_grid.astype(F32) / 1048576.0
    masses = source_weight.astype(F32) / 16.0
    offset = jnp.log2(masses) - RATE2 * jnp.sum(points * points, axis=0, keepdims=True)
    payload = jnp.concatenate([points, offset, jnp.zeros((7, points.shape[1]), F32)], axis=0)
    spread = jnp.broadcast_to(payload[None], (BLOCKS,) + payload.shape)
    near = lax.all_to_all(spread, ("z", "x"), 0, 0, tiled=True)
    far = lax.ppermute(near, "core", [(0, 1), (1, 0)])
    stack = ((ROWS, 256), BF16)
    part, near_left, right = run(
        near_kernel, 6, [((1, 1536), F32), stack, ((512, 1536), BF16)],
        (near, *tgts),
    )
    *parts, far_left = run(far_kernel, 6, [((1, 512), F32)] * 3 + [stack], (far, right, part))
    total = run(
        own_kernel, 4, [((1, 512), F32)], (near_left, far_left, targets),
        [pltpu.VMEM((512, 512), BF16)],
    )[0]
    for part, k in zip(parts, SHIFTS):
        part = along_y(part, 4 - k)
        total = total + part
    return total.reshape(512)


def solution(mesh):
    torus = Mesh(mesh.devices.reshape(2, 2, 4, 4, 2), NAMES)
    specs = (P(None, NAMES),) * 3
    return jax.shard_map(shards, mesh=torus, in_specs=specs, out_specs=P(NAMES), check_vma=False)
```
